32 devices in a mesh: blk: 8 (over z, core), bond: 4 (over y, x).
Axes of the slice: x: 2, y: 2, z: 4, core: 2. Of those that a mesh axis runs over, the one named last changes fastest.
Arguments:
- iso: bfloat16 [8, 256, 256, 256], P('blk', None, 'bond'), may hold values from -0.03125 to 0.03125
- edge_left: bfloat16 [8, 256, 256], P('blk'), may hold values from -0.375 to 0.375
- edge_right: bfloat16 [8, 256, 256], P('blk'), may hold values from -0.375 to 0.375
- coupling: float32 [8, 256, 256], P('blk'), may hold values from -0.25 to 0.25
Outputs:
- iso_out: bfloat16 [8, 256, 256, 256], P('blk', None, 'bond')
- top_env: float32 [8, 256, 256], P('blk')
The draws below stay inside these ranges and needn't reach their ends.
All inputs are finite; a program needn't handle non-finite values.
Results may differ from the reference program's by a relative error of at most 0.00105.
The reference program's roundings to bfloat16 on the way count: a program that leaves them out, or rounds other values in their place, can miss the bound.
Values may be sent and summed in bfloat16 or wider, within the bound.
A program may use at most 128 MiB of HBM per device.

```python
import math
import jax
import jax.numpy as jnp
from jax import lax

CHI = 256
NEWTON = 2
SUBTREES = 8
LEVELS = 3
CB = 64


def draw_iso(key, part):
    ranks = 4
    sigma = 1.0 / CHI
    block_ids = jnp.arange(CHI, dtype=jnp.int32) // CB
    block_weights = jax.random.uniform(jax.random.fold_in(key, 7001), (ranks, CHI // CB), jnp.float32, 0.0, 1.0)
    per_column = jnp.take(block_weights, block_ids, axis=1)
    strength = 0.5

    def one_subtree(index):
        subkey = jax.random.fold_in(jax.random.fold_in(key, 7002), index)
        first_key, second_key, third_key = jax.random.split(subkey, 3)
        base = jnp.clip(jax.random.normal(first_key, (CHI, CHI, CHI), jnp.float32), -6.0, 6.0)
        shared = jax.random.normal(second_key, (ranks, CHI, CHI), jnp.float32) * per_column[:, None, :]
        columns = jax.random.normal(third_key, (ranks, CHI), jnp.float32)
        common = jnp.einsum('rab,rp->abp', shared, columns) * (strength / math.sqrt(ranks))
        values = jnp.clip(sigma * (base + common), -8.0 * sigma, 8.0 * sigma)
        return values.astype(jnp.bfloat16)
    return lax.map(one_subtree, jnp.arange(SUBTREES, dtype=jnp.int32))


def block_scale(own_key, extent, cuts, smallest, top_value):
    loudness, own = 1.0, jax.random.fold_in(own_key, 6)
    for position, shards_of in cuts:
        draws = jnp.exp(jax.random.uniform(jax.random.fold_in(own, position), (shards_of,), jnp.float32, smallest / len(cuts), top_value / len(cuts)))
        loudness = loudness * jnp.repeat(draws, extent[position] // shards_of).reshape([-1 if axis == position else 1 for axis in range(len(extent))])
    return loudness


def normal_values(own_key, shape, width, reach, pieces=(), held_as=jnp.bfloat16):
    entries = width * jax.random.normal(own_key, shape, jnp.float32)
    if pieces:
        entries = entries * block_scale(own_key, shape, pieces, -0.22, 0.18)
    return jnp.clip(entries, -reach, reach).astype(held_as)


def setup_inputs(seed: int = 0) -> dict:
    key_of = jax.random.split(jax.random.key(seed), 5)
    iso = draw_iso(jax.random.fold_in(key_of[4], 71), 0)
    edge_left = normal_values(key_of[1], (SUBTREES, CHI, CHI), CHI ** -0.5, 0.375, ((0, 8),))
    edge_right = normal_values(key_of[2], (SUBTREES, CHI, CHI), CHI ** -0.5, 0.375, ((0, 8),))
    coupling = normal_values(key_of[3], (SUBTREES, CHI, CHI), (2 * CHI) ** -0.5, 0.25, ((0, 8),), jnp.float32)
    return {"iso": iso, "edge_left": edge_left, "edge_right": edge_right, "coupling": coupling}


highest = lax.Precision.HIGHEST

def ascend_pair(packed):
    iso_one, left_one, right_one = packed
    wide_iso = iso_one.astype(jnp.float32)
    operators = jnp.stack([left_one, right_one]).astype(jnp.float32)
    mapped = jnp.einsum('kxa,abp->kxbp', operators, wide_iso, precision=highest)
    return jnp.einsum('abp,kabq->kpq', wide_iso, mapped, precision=highest)

def update_one(packed):
    iso_one, mix_one, top_one = packed
    wide_iso = iso_one.astype(jnp.float32)
    gradient = jnp.einsum('xa,abp->xbp', mix_one.astype(jnp.float32), wide_iso, precision=highest)
    gradient = gradient + jnp.einsum('abq,qp->abp', wide_iso, top_one.astype(jnp.float32), precision=highest)
    flattened = gradient.reshape(CHI * CHI, CHI)
    flattened = flattened * lax.rsqrt(jnp.sum(flattened * flattened) + 1e-06)
    for newton_step in range(NEWTON):
        gram_mat = jnp.dot(flattened.T, flattened, precision=highest)
        flattened = 1.5 * flattened - 0.5 * jnp.dot(flattened, gram_mat, precision=highest)
    return flattened.reshape(CHI, CHI, CHI).astype(jnp.bfloat16)

def reference(iso, edge_left, edge_right, coupling):
    ascended = lax.map(ascend_pair, (iso, edge_left, edge_right)).astype(jnp.bfloat16)
    left_bounds = ascended[:, 0]
    right_bounds = ascended[:, 1]
    environ = left_bounds.astype(jnp.float32) + right_bounds.astype(jnp.float32)
    subtree_ids = jnp.arange(SUBTREES, dtype=jnp.int32)
    for level_idx in range(LEVELS):
        partner = environ[jnp.bitwise_xor(subtree_ids, 1 << level_idx)]
        mapped = jnp.einsum('sij,sjk,slk->sil', coupling, partner, coupling, precision=highest)
        environ = 0.5 * (environ + mapped)
    top_low = environ.astype(jnp.bfloat16)
    mixed_op = edge_left.astype(jnp.float32) + jnp.roll(right_bounds, 1, axis=0).astype(jnp.float32)
    mixed_op = (mixed_op + jnp.roll(left_bounds, -1, axis=0).astype(jnp.float32)).astype(jnp.bfloat16)
    iso_out = lax.map(update_one, (iso, mixed_op, top_low))
    return (iso_out, environ)
```

```python
import functools

import jax
import jax.numpy as jnp
from jax import lax
from jax.experimental import pallas as pl
from jax.experimental.pallas import tpu as pltpu
from jax.sharding import PartitionSpec as P

NEWTON = 2
CHUNK = 16
GROUP = 4
SLAB = 8

highest = lax.Precision.HIGHEST
f32 = jnp.float32
bf16 = jnp.bfloat16
MESH = pl.DeviceIdType.MESH


def mm(a, b):
    return jnp.dot(a, b, preferred_element_type=f32)


def exact(a, b):
    return jnp.dot(a, b, precision=highest, preferred_element_type=f32)


def exact_turned(a, b):
    return lax.dot_general(
        a, b, (((1,), (1,)), ((), ())), precision=highest, preferred_element_type=f32
    )


def diagonal(shape):
    return lax.broadcasted_iota(jnp.int32, shape, 0) == lax.broadcasted_iota(jnp.int32, shape, 1)


def flipped(index, mask):
    out = index
    bit = 1
    while bit <= mask:
        if mask & bit:
            out = out + bit * (1 - 2 * lax.rem(index // bit, 2))
        bit *= 2
    return out


def halves(value):
    high = value.astype(bf16)
    return high, (value - high.astype(f32)).astype(bf16)


def sweep_kernel(
    blk, bond, levels,
    iso_ref, left_ref, right_ref, couple_ref,
    rows_out, mix_out, top_out, env_out, gram_out, trace_out,
    stage, even, odd, total, heard, asc, around, other, mixed, envs, far, grams, packed, traces,
    in_sem, out_sem, rs_send, rs_recv, ag_send, ag_recv, nb_send, nb_recv, zero_send, zero_recv,
    mix_send, mix_recv, dir_send, dir_recv, fw_send, fw_recv, gr_send, gr_recv, tr_send, tr_recv,
):
    s = lax.axis_index("blk")
    r = lax.axis_index("bond")
    chi = left_ref.shape[0]
    chunks = stage.shape[0]
    half = chunks // 2
    piece = chi // bond
    square = (chi, chi)
    cut = (bond, piece, chi)
    after = lax.rem(s + 1, blk)
    before = lax.rem(s + blk - 1, blk)
    masks = range(1, bond)
    pending = []

    loads = [
        pltpu.make_async_copy(iso_ref.at[:, pl.ds(SLAB * c, SLAB), :], stage.at[c], in_sem.at[c])
        for c in range(chunks)
    ]
    for load in loads:
        load.start()

    barrier = pltpu.get_barrier_semaphore()
    partners = [flipped(s, 1 << level) for level in range(levels)]
    greeted = [(s, flipped(r, mask)) for mask in masks]
    greeted += [(after, r), (before, r)] + [(t, r) for t in partners]
    for device in greeted:
        pl.semaphore_signal(barrier, inc=1, device_id=device, device_id_type=MESH)

    def send(src, dst, out_flag, in_flag, device):
        copy = pltpu.make_async_remote_copy(
            src_ref=src, dst_ref=dst, send_sem=out_flag, recv_sem=in_flag,
            device_id=device, device_id_type=MESH,
        )
        copy.start()
        pending.append(copy)
        return copy

    def relayout(c, dst, i):
        dst[i] = jnp.transpose(stage[c], (1, 0, 2))

    def ascend(k, edge_ref, src, i):
        for first in range(0, SLAB, GROUP):
            mats = [src[i, first + j] for j in range(GROUP)]
            turned = jnp.concatenate(mats, axis=0).T
            both = jnp.concatenate([mm(edge_ref[...], one) for one in mats], axis=0)
            high, low = halves(both)
            total[k] += (mm(turned, high) + mm(turned, low)).reshape(cut)

    total[...] = jnp.zeros_like(total)
    grams[...] = jnp.zeros_like(grams)
    loads[0].wait()
    relayout(0, even, 0)

    def load_wait(c):
        pltpu.make_async_copy(
            iso_ref.at[:, pl.ds(0, SLAB), :], stage.at[c], in_sem.at[c]
        ).wait()

    def first_pass(i, carry):
        load_wait(2 * i + 1)
        relayout(2 * i + 1, odd, i)
        ascend(0, left_ref, even, i)

        @pl.when(i + 1 < half)
        def _():
            load_wait(2 * i + 2)

        relayout(lax.rem(2 * i + 2, chunks), even, i + 1)
        ascend(0, left_ref, odd, i)
        return carry

    lax.fori_loop(0, half, first_pass, 0)
    pl.semaphore_wait(barrier, len(greeted))

    def scatter(k):
        return [
            send(total.at[k, flipped(r, mask)], heard.at[k, mask - 1],
                 rs_send.at[k, mask - 1], rs_recv.at[k, mask - 1], (s, flipped(r, mask)))
            for mask in masks
        ]

    def gather(k):
        return [
            send(asc.at[k, r], asc.at[k, r], ag_send.at[k, mask - 1], ag_recv.at[k, mask - 1],
                 (s, flipped(r, mask)))
            for mask in masks
        ]

    def reduced(k, copies):
        for copy in copies:
            copy.wait_recv()
        own = total[k, r]
        for mask in masks:
            own = own + heard[k, mask - 1]
        asc[k, r] = own.astype(bf16)

    def arrived(copies):
        for copy in copies:
            copy.wait_recv()

    def second_pass(i, carry):
        ascend(1, right_ref, even, i)
        ascend(1, right_ref, odd, i)
        return carry

    scattered_left = scatter(0)
    early = half * 3 // 4
    lax.fori_loop(0, early, second_pass, 0)
    reduced(0, scattered_left)
    gathered_left = gather(0)
    to_before = send(asc.at[0, r], around.at[0], nb_send.at[0], nb_recv.at[0], (before, r))
    lax.fori_loop(early, half, second_pass, 0)
    scattered_right = scatter(1)

    stores = []
    for c in range(chunks):
        src = (odd if c % 2 else even).at[c // 2]
        store = pltpu.make_async_copy(src, rows_out.at[pl.ds(SLAB * c, SLAB)], out_sem.at[c])
        store.start()
        stores.append(store)

    def plain_pass(i, carry):
        for src in (even, odd):
            for first in range(0, SLAB, GROUP):
                rows = jnp.concatenate([src[i, first + j] for j in range(GROUP)], axis=0)
                grams[2] += mm(rows.T, rows)
        return carry

    lax.fori_loop(0, half, plain_pass, 0)
    arrived(gathered_left)
    zero_left = send(asc.at[0], other.at[0], zero_send.at[0], zero_recv.at[0], (partners[0], r))
    reduced(1, scattered_right)
    gathered_right = gather(1)
    to_after = send(asc.at[1, r], around.at[1], nb_send.at[1], nb_recv.at[1], (after, r))
    arrived(gathered_right)
    zero_right = send(asc.at[1], other.at[1], zero_send.at[1], zero_recv.at[1], (partners[0], r))
    envs[0] = asc[0].astype(f32) + asc[1].astype(f32)
    arrived([to_before, to_after])
    mine = left_ref[pl.ds(pl.multiple_of(r * piece, piece), piece), :].astype(f32)
    mixed[r] = (mine + around[1].astype(f32) + around[0].astype(f32)).astype(bf16)
    gathered_mix = [
        send(mixed.at[r], mixed.at[r], mix_send.at[mask - 1], mix_recv.at[mask - 1],
             (s, flipped(r, mask)))
        for mask in masks
    ]

    def climb(level, partner):
        couple = couple_ref[...]
        carried = exact_turned(exact(couple, partner.reshape(square)), couple)
        envs[level + 1] = 0.5 * (envs[level] + carried.reshape(cut))

    arrived([zero_left, zero_right])
    climb(0, other[0].astype(f32) + other[1].astype(f32))

    def gram_pass(i, carry):
        mix = mixed[...].reshape(square)
        for src in (even, odd):
            for first in range(0, SLAB, GROUP):
                mats = [src[i, first + j] for j in range(GROUP)]
                rows = jnp.concatenate(mats, axis=0)
                moved = jnp.concatenate([mm(mix, one).astype(bf16) for one in mats], axis=0)
                turned = moved.T
                grams[0] += mm(turned, moved)
                grams[1] += mm(turned, rows)
        return carry

    slots = 2 * (levels - 1)

    def gram_slot(slot):
        lax.fori_loop(slot * half // slots, (slot + 1) * half // slots, gram_pass, 0)

    opposite = bond - 1
    for level in range(1, levels):
        target = (partners[level], r)
        direct = [
            send(envs.at[level, place], far.at[level - 1, place],
                 dir_send.at[level - 1, n], dir_recv.at[level - 1, n], target)
            for n, place in enumerate((r, flipped(r, opposite)))
        ]
        if level == 1:
            arrived(gathered_mix)
        gram_slot(2 * (level - 1))
        direct[0].wait_recv()
        passed = [
            send(far.at[level - 1, r], far.at[level - 1, r],
                 fw_send.at[level - 1, mask - 1], fw_recv.at[level - 1, mask - 1],
                 (s, flipped(r, mask)))
            for mask in masks if mask != opposite
        ]
        gram_slot(2 * (level - 1) + 1)
        direct[1].wait_recv()
        arrived(passed)
        climb(level, far[level - 1])

    env = envs[levels].reshape(square)
    top = env.astype(bf16)
    wide = top.astype(f32)
    crossed = exact(grams[1] + 0.5 * exact(wide.T, grams[2]), wide)
    gram = grams[0] + crossed + crossed.T
    packed[r] = gram.astype(bf16)
    trace = jnp.sum(jnp.where(diagonal(gram.shape), gram, 0.0), keepdims=True)
    traces[r] = jnp.broadcast_to(trace, traces.shape[1:])
    gathered_gram = []
    for mask in masks:
        device = (s, flipped(r, mask))
        gathered_gram.append(send(
            packed.at[r], packed.at[r], gr_send.at[mask - 1], gr_recv.at[mask - 1], device))
        gathered_gram.append(send(
            traces.at[r], traces.at[r], tr_send.at[mask - 1], tr_recv.at[mask - 1], device))
    env_out[...] = env
    top_out[...] = top
    mix_out[...] = mixed[...].reshape(square)
    for store in stores:
        store.wait()
    arrived(gathered_gram)
    gram_out[...] = packed[...]
    trace_out[...] = traces[...]
    for copy in pending:
        copy.wait_send()


def update_kernel(
    rows_ref, mix_ref, top_ref, env_ref, gram_ref, trace_ref, out_ref, env_out,
    held_ref, rest_ref, mean_ref,
):
    @pl.when(pl.program_id(0) == 0)
    def _():
        env_out[...] = env_ref[...]
        gram = gram_ref[0].astype(f32)
        squares = trace_ref[0]
        for rank in range(1, gram_ref.shape[0]):
            gram = gram + gram_ref[rank].astype(f32)
            squares = squares + trace_ref[rank]
        scale = lax.rsqrt(squares[0:1, 0:1] + 1e-06)
        first_gram = gram * (scale * scale)
        gram = first_gram
        eye = diagonal(gram.shape).astype(f32)
        total = eye
        for newton_step in range(NEWTON):
            step = 1.5 * eye - 0.5 * gram
            total = step if newton_step == 0 else exact(total, step)
            if newton_step + 1 < NEWTON:
                gram = exact(exact(step, gram), step)
        energy = jnp.sum(first_gram * eye, keepdims=True)
        mean = jnp.sum(first_gram * total, keepdims=True) / jnp.maximum(energy, 1e-30)
        rest_ref[...] = ((total - mean * eye) * scale).astype(bf16)
        mean_ref[...] = jnp.broadcast_to(mean * scale, mean_ref.shape)

    mean = mean_ref[...]

    def step(g, carry):
        mats = [rows_ref[g * GROUP + j] for j in range(GROUP)]
        rows = jnp.concatenate(mats, axis=0)
        moved = jnp.concatenate([mm(mix_ref[...], one) for one in mats], axis=0)
        grad = moved + mm(rows, top_ref[...])
        done = (mean * grad + mm(grad.astype(bf16), rest_ref[...])).astype(bf16)
        held_ref[pl.ds(g * GROUP, GROUP)] = done.reshape(GROUP, *mix_ref.shape)
        return carry

    lax.fori_loop(0, rows_ref.shape[0] // GROUP, step, 0, unroll=2)
    out_ref[...] = jnp.transpose(held_ref[...], (1, 0, 2))


def whole(shape):
    return pl.BlockSpec(shape, lambda i: (0,) * len(shape))


def body(iso, edge_left, edge_right, coupling):
    iso = iso[0]
    chi, depth, _ = iso.shape
    blk = lax.axis_size("blk")
    bond = lax.axis_size("bond")
    levels = blk.bit_length() - 1
    square = (chi, chi)
    piece = chi // bond
    chunks = depth // SLAB
    half = chunks // 2
    work = 2 * depth * chi**3
    dma = pltpu.SemaphoreType.DMA
    vmem = pl.BlockSpec(memory_space=pltpu.VMEM)
    hbm = pl.BlockSpec(memory_space=pl.ANY)
    rows, mix, top, environ, grams, traces = pl.pallas_call(
        functools.partial(sweep_kernel, blk, bond, levels),
        in_specs=[hbm, vmem, vmem, vmem],
        out_specs=[hbm] + [vmem] * 5,
        out_shape=[
            jax.ShapeDtypeStruct((depth, *square), bf16),
            jax.ShapeDtypeStruct(square, bf16),
            jax.ShapeDtypeStruct(square, bf16),
            jax.ShapeDtypeStruct(square, f32),
            jax.ShapeDtypeStruct((bond, *square), bf16),
            jax.ShapeDtypeStruct((bond, 8, 128), f32),
        ],
        scratch_shapes=[
            pltpu.VMEM((chunks, chi, SLAB, chi), bf16),
            pltpu.VMEM((half + 1, SLAB, *square), bf16),
            pltpu.VMEM((half, SLAB, *square), bf16),
            pltpu.VMEM((2, bond, piece, chi), f32),
            pltpu.VMEM((2, bond - 1, piece, chi), f32),
            pltpu.VMEM((2, bond, piece, chi), bf16),
            pltpu.VMEM((2, piece, chi), bf16),
            pltpu.VMEM((2, bond, piece, chi), bf16),
            pltpu.VMEM((bond, piece, chi), bf16),
            pltpu.VMEM((levels + 1, bond, piece, chi), f32),
            pltpu.VMEM((levels - 1, bond, piece, chi), f32),
            pltpu.VMEM((3, *square), f32),
            pltpu.VMEM((bond, *square), bf16),
            pltpu.VMEM((bond, 8, 128), f32),
            dma((chunks,)), dma((chunks,)),
            dma((2, bond - 1)), dma((2, bond - 1)),
            dma((2, bond - 1)), dma((2, bond - 1)),
            dma((2,)), dma((2,)), dma((2,)), dma((2,)),
            dma((bond - 1,)), dma((bond - 1,)),
            dma((levels - 1, 2)), dma((levels - 1, 2)),
            dma((levels - 1, bond - 1)), dma((levels - 1, bond - 1)),
            dma((bond - 1,)), dma((bond - 1,)),
            dma((bond - 1,)), dma((bond - 1,)),
        ],
        compiler_params=pltpu.CompilerParams(
            vmem_limit_bytes=48 * 1024 * 1024, collective_id=0, has_side_effects=True
        ),
        cost_estimate=pl.CostEstimate(flops=10 * work, bytes_accessed=4 * iso.size, transcendentals=0),
        name="sweep",
    )(iso, edge_left[0], edge_right[0], coupling[0])
    chunk = CHUNK if depth % CHUNK == 0 else depth
    iso_spec = pl.BlockSpec((chi, chunk, chi), lambda i: (0, i, 0))
    rows_spec = pl.BlockSpec((chunk, chi, chi), lambda i: (i, 0, 0))
    updated, environ = pl.pallas_call(
        update_kernel,
        grid=(depth // chunk,),
        in_specs=[rows_spec] + [whole(square)] * 3 + [whole(grams.shape), whole(traces.shape)],
        out_specs=[iso_spec, whole(square)],
        out_shape=[
            jax.ShapeDtypeStruct(iso.shape, bf16),
            jax.ShapeDtypeStruct(square, f32),
        ],
        scratch_shapes=[
            pltpu.VMEM((chunk, *square), bf16),
            pltpu.VMEM(square, bf16),
            pltpu.VMEM((1, chi), f32),
        ],
        compiler_params=pltpu.CompilerParams(
            dimension_semantics=("arbitrary",), vmem_limit_bytes=48 * 1024 * 1024
        ),
        cost_estimate=pl.CostEstimate(flops=3 * work, bytes_accessed=4 * iso.size, transcendentals=0),
        name="update",
    )(rows, mix, top, environ, grams, traces)
    return (updated[None], environ[None])


def solution(mesh):
    placed = (
        P("blk", None, "bond", None),
        P("blk", None, None),
        P("blk", None, None),
        P("blk", None, None),
    )
    return jax.shard_map(
        body,
        mesh=mesh,
        in_specs=placed,
        out_specs=(P("blk", None, "bond", None), P("blk", None, None)),
        check_vma=False,
    )
```

```python
import functools

import jax
import jax.numpy as jnp
from jax import lax
from jax.experimental import pallas as pl
from jax.experimental.pallas import tpu as pltpu
from jax.sharding import PartitionSpec as P

GROUP = 4
SLAB = 8
SWEEP_VMEM = 61 * 1024 * 1024
UPDATE_VMEM = 61 * 1024 * 1024

highest = lax.Precision.HIGHEST
f32 = jnp.float32
bf16 = jnp.bfloat16
MESH = pl.DeviceIdType.MESH


def mm(a, b):
    return jnp.dot(a, b, preferred_element_type=f32)


def exact(a, b):
    return jnp.dot(a, b, precision=highest, preferred_element_type=f32)


def exact_turned(a, b):
    return lax.dot_general(
        a, b, (((1,), (1,)), ((), ())), precision=highest, preferred_element_type=f32
    )


def diagonal(shape):
    return lax.broadcasted_iota(jnp.int32, shape, 0) == lax.broadcasted_iota(jnp.int32, shape, 1)


def flipped(index, mask):
    out = index
    bit = 1
    while bit <= mask:
        if mask & bit:
            out = out + bit * (1 - 2 * lax.rem(index // bit, 2))
        bit *= 2
    return out


def halves(value):
    high = value.astype(bf16)
    return high, (value - high.astype(f32)).astype(bf16)


def sweep_kernel(
    blk, bond, levels,
    iso_ref, left_in, right_in, couple_in,
    grad_out, env_out, gram_out, trace_out,
    left_ref, right_ref, couple_ref, grad, stage, even, odd, turn_even, turn_odd,
    high_even, low_even, high_odd, low_odd, total, heard, asc, around, other, mixed, envs, far, grams, packed, traces,
    in_sem, small_sem, grad_sem, tail_sem, rs_send, rs_recv, ag_send, ag_recv, nb_send, nb_recv, zero_send, zero_recv,
    mix_send, mix_recv, dir_send, dir_recv, fw_send, fw_recv, gr_send, gr_recv, tr_send, tr_recv,
):
    s = lax.axis_index("blk")
    r = lax.axis_index("bond")
    chi = left_ref.shape[0]
    chunks = iso_ref.shape[1] // SLAB
    slots_in = stage.shape[0]
    half = chunks // 2
    piece = chi // bond
    square = (chi, chi)
    cut = (bond, piece, chi)
    after = lax.rem(s + 1, blk)
    before = lax.rem(s + blk - 1, blk)
    masks = range(1, bond)
    pending = []

    def load(c):
        slot = lax.rem(c, slots_in)
        first = c * SLAB if isinstance(c, int) else pl.multiple_of(c * SLAB, SLAB)
        return pltpu.make_async_copy(
            iso_ref.at[:, pl.ds(first, SLAB), :], stage.at[slot], in_sem.at[slot]
        )

    small = [
        pltpu.make_async_copy(src, dst, small_sem.at[n])
        for n, (src, dst) in enumerate(
            ((left_in, left_ref), (right_in, right_ref), (couple_in, couple_ref))
        )
    ]
    load(0).start()
    for copy in small:
        copy.start()
    load(1).start()

    barrier = pltpu.get_barrier_semaphore()
    partners = [flipped(s, 1 << level) for level in range(levels)]
    greeted = [(s, flipped(r, mask)) for mask in masks]
    greeted += [(after, r), (before, r)] + [(t, r) for t in partners]
    for device in greeted:
        pl.semaphore_signal(barrier, inc=1, device_id=device, device_id_type=MESH)

    def send(src, dst, out_flag, in_flag, device):
        copy = pltpu.make_async_remote_copy(
            src_ref=src, dst_ref=dst, send_sem=out_flag, recv_sem=in_flag,
            device_id=device, device_id_type=MESH,
        )
        copy.start()
        pending.append(copy)
        return copy

    def relayout(c, dst, i):
        dst[i] = jnp.transpose(stage[lax.rem(c, slots_in)], (1, 0, 2))

    def spread(edge_ref, src, i, turn, high, low):
        for j in range(SLAB):
            one = src[i, j]
            place = slice(j * chi, (j + 1) * chi)
            high[place, :], low[place, :] = halves(mm(edge_ref[...], one))
            if turn is not None:
                turn[i, :, place] = one.T

    def collect(k, turn, i, high, low):
        turned = turn[i]
        total[k] += (mm(turned, high[...]) + mm(turned, low[...])).reshape(cut)

    even_parts = (high_even, low_even)
    odd_parts = (high_odd, low_odd)
    total[...] = jnp.zeros_like(total)
    grams[...] = jnp.zeros_like(grams)
    load(0).wait()
    for c in range(2, min(4, chunks)):
        load(c).start()
    for copy in small:
        copy.wait()
    relayout(0, even, 0)
    spread(left_ref, even, 0, turn_even, *even_parts)
    load(1).wait()
    relayout(1, odd, 0)

    def first_pass(i, carry):
        for ahead in (2, 3):
            @pl.when(2 * i + ahead < chunks)
            def _():
                load(2 * i + ahead).wait()

            @pl.when(2 * i + ahead + 2 < chunks)
            def _():
                load(2 * i + ahead + 2).start()

        collect(0, turn_even, i, *even_parts)
        spread(left_ref, odd, i, turn_odd, *odd_parts)
        relayout(2 * i + 2, even, i + 1)
        collect(0, turn_odd, i, *odd_parts)
        spread(left_ref, even, i + 1, turn_even, *even_parts)
        relayout(2 * i + 3, odd, i + 1)
        return carry

    with jax.named_scope('first'):
        lax.fori_loop(0, half, first_pass, 0)
    pl.semaphore_wait(barrier, len(greeted))

    def scatter(k):
        return [
            send(total.at[k, flipped(r, mask)], heard.at[k, mask - 1],
                 rs_send.at[k, mask - 1], rs_recv.at[k, mask - 1], (s, flipped(r, mask)))
            for mask in masks
        ]

    def gather(k):
        return [
            send(asc.at[k, r], asc.at[k, r], ag_send.at[k, mask - 1], ag_recv.at[k, mask - 1],
                 (s, flipped(r, mask)))
            for mask in masks
        ]

    def reduced(k, copies):
        for copy in copies:
            copy.wait_recv()
        own = total[k, r]
        for mask in masks:
            own = own + heard[k, mask - 1]
        asc[k, r] = own.astype(bf16)

    def arrived(copies):
        for copy in copies:
            copy.wait_recv()

    def second_pass(i, carry):
        collect(1, turn_even, i, *even_parts)
        spread(right_ref, odd, i, None, *odd_parts)
        collect(1, turn_odd, i, *odd_parts)
        spread(right_ref, even, i + 1, None, *even_parts)
        return carry

    scattered_left = scatter(0)
    spread(right_ref, even, 0, None, *even_parts)
    early = half * 3 // 4
    with jax.named_scope('second_a'):
        lax.fori_loop(0, early, second_pass, 0)
    with jax.named_scope('w_rs0'):
        reduced(0, scattered_left)
    gathered_left = gather(0)
    to_before = send(asc.at[0, r], around.at[0], nb_send.at[0], nb_recv.at[0], (before, r))
    with jax.named_scope('second_b'):
        lax.fori_loop(early, half, second_pass, 0)
    scattered_right = scatter(1)

    def plain_pass(i, carry):
        for src, turn in ((even, turn_even), (odd, turn_odd)):
            grams[2] += mm(turn[i], src[i].reshape(SLAB * chi, chi))
        return carry

    plain_early = half // 2
    with jax.named_scope('plain'):
        lax.fori_loop(0, plain_early, plain_pass, 0)
    with jax.named_scope('w_ag0'):
        arrived(gathered_left)
    zero_left = send(asc.at[0], other.at[0], zero_send.at[0], zero_recv.at[0], (partners[0], r))
    with jax.named_scope('w_rs1'):
        reduced(1, scattered_right)
    gathered_right = gather(1)
    to_after = send(asc.at[1, r], around.at[1], nb_send.at[1], nb_recv.at[1], (after, r))
    with jax.named_scope('w_ag1'):
        arrived(gathered_right)
    zero_right = send(asc.at[1], other.at[1], zero_send.at[1], zero_recv.at[1], (partners[0], r))
    envs[0] = asc[0].astype(f32) + asc[1].astype(f32)
    def climb(level, partner):
        couple = couple_ref[...]
        carried = exact_turned(exact(couple, partner.reshape(square)), couple)
        envs[level + 1] = 0.5 * (envs[level] + carried.reshape(cut))

    with jax.named_scope('w_zero'):
        arrived([zero_left, zero_right])
    with jax.named_scope('climb0'):
        climb(0, other[0].astype(f32) + other[1].astype(f32))
    opposite = bond - 1

    def send_direct(level):
        return [
            send(envs.at[level, place], far.at[level - 1, place],
                 dir_send.at[level - 1, n], dir_recv.at[level - 1, n], (partners[level], r))
            for n, place in enumerate((r, flipped(r, opposite)))
        ]

    direct = send_direct(1)
    with jax.named_scope('w_nb'):
        arrived([to_before, to_after])
    mine = left_ref[pl.ds(pl.multiple_of(r * piece, piece), piece), :].astype(f32)
    mixed[r] = (mine + around[1].astype(f32) + around[0].astype(f32)).astype(bf16)
    gathered_mix = [
        send(mixed.at[r], mixed.at[r], mix_send.at[mask - 1], mix_recv.at[mask - 1],
             (s, flipped(r, mask)))
        for mask in masks
    ]

    def gram_pass(i, carry):
        mix = mixed[...].reshape(square)
        for src in (even, odd):
            for first in range(0, SLAB, GROUP):
                mats = [src[i, first + j] for j in range(GROUP)]
                rows = jnp.concatenate(mats, axis=0)
                moved = jnp.concatenate([mm(mix, one).astype(bf16) for one in mats], axis=0)
                turned = moved.T
                grams[0] += mm(turned, moved)
                grams[1] += mm(turned, rows)
        return carry

    shares = 2 * (levels - 1) - 1

    def gram_share(n):
        lax.fori_loop(n * half // shares, (n + 1) * half // shares, gram_pass, 0)

    for level in range(1, levels):
        if level == 1:
            with jax.named_scope('plain_late'):
                lax.fori_loop(plain_early, half, plain_pass, 0)
        else:
            direct = send_direct(level)
            with jax.named_scope('slot_a'):
                gram_share(2 * level - 3)
        with jax.named_scope('w_dir'):
            direct[0].wait_recv()
        passed = [
            send(far.at[level - 1, r], far.at[level - 1, r],
                 fw_send.at[level - 1, mask - 1], fw_recv.at[level - 1, mask - 1],
                 (s, flipped(r, mask)))
            for mask in masks if mask != opposite
        ]
        if level == 1:
            with jax.named_scope('w_mix'):
                arrived(gathered_mix)
        with jax.named_scope('slot_b'):
            gram_share(2 * level - 2)
        with jax.named_scope('w_dir1'):
            direct[1].wait_recv()
        with jax.named_scope('w_fw'):
            arrived(passed)
        with jax.named_scope('climb'):
            climb(level, far[level - 1])

    env = envs[levels].reshape(square)
    top = env.astype(bf16)
    wide = top.astype(f32)
    crossed = exact(grams[1] + 0.5 * exact(wide.T, grams[2]), wide)
    gram = grams[0] + crossed + crossed.T
    low = chi // 2
    packed[r] = jnp.concatenate([gram[:low], gram[low:, low:]], axis=1).astype(bf16)
    trace = jnp.sum(jnp.where(diagonal(gram.shape), gram, 0.0), keepdims=True)
    traces[r] = jnp.broadcast_to(trace, traces.shape[1:])
    gathered_gram = []
    for mask in masks:
        device = (s, flipped(r, mask))
        gathered_gram.append(send(
            packed.at[r], packed.at[r], gr_send.at[mask - 1], gr_recv.at[mask - 1], device))
        gathered_gram.append(send(
            traces.at[r], traces.at[r], tr_send.at[mask - 1], tr_recv.at[mask - 1], device))
    tails = [pltpu.make_async_copy(envs.at[levels], env_out, tail_sem.at[0])]
    tails[0].start()

    def grad_pass(i, carry):
        mix = mixed[...].reshape(square)
        for n, src in enumerate((even, odd)):
            for first in range(0, SLAB, GROUP):
                mats = [src[i, first + j] for j in range(GROUP)]
                rows = jnp.concatenate(mats, axis=0)
                moved = jnp.concatenate([mm(mix, one) for one in mats], axis=0)
                grad[2 * i + n, first:first + GROUP] = (moved + mm(rows, top)).reshape(GROUP, *square)
            pltpu.make_async_copy(
                grad.at[2 * i + n], grad_out.at[2 * i + n], grad_sem.at[2 * i + n]
            ).start()
        return carry

    with jax.named_scope('grad'):
        lax.fori_loop(0, half, grad_pass, 0)
    with jax.named_scope('w_gram'):
        arrived(gathered_gram)
    for n, (src, dst) in enumerate(((packed, gram_out), (traces, trace_out))):
        tails.append(pltpu.make_async_copy(src, dst, tail_sem.at[n + 1]))
        tails[-1].start()
    for copy in tails:
        copy.wait()
    for c in range(chunks):
        pltpu.make_async_copy(grad.at[c], grad_out.at[c], grad_sem.at[c]).wait()
    for copy in pending:
        copy.wait_send()


def update_kernel(
    grad_ref, env_ref, gram_ref, trace_ref, out_ref, env_out,
    grads, env, grams, traces, held, in_sem, out_sem, tail_sem,
):
    def load(c):
        return pltpu.make_async_copy(grad_ref.at[c], grads.at[c], in_sem.at[c])

    gram_copy = pltpu.make_async_copy(gram_ref, grams, tail_sem.at[0])
    trace_copy = pltpu.make_async_copy(trace_ref, traces, tail_sem.at[1])
    env_in = pltpu.make_async_copy(env_ref, env, tail_sem.at[2])
    env_back = pltpu.make_async_copy(env, env_out, tail_sem.at[3])
    gram_copy.start()
    trace_copy.start()
    for c in range(grads.shape[0]):
        load(c).start()
    env_in.start()
    chi = out_ref.shape[0]
    low = chi // 2
    gram_copy.wait()
    trace_copy.wait()
    packed = grams[0].astype(f32)
    squares = traces[0]
    for rank in range(1, grams.shape[0]):
        packed = packed + grams[rank].astype(f32)
        squares = squares + traces[rank]
    scale = lax.rsqrt(squares[0:1, 0:1] + 1e-06)
    under = jnp.concatenate([packed[:, low:chi].T, packed[:, chi:]], axis=1)
    gram = jnp.concatenate([packed[:, :chi], under], axis=0) * (scale * scale)
    eye = diagonal(gram.shape).astype(f32)
    twice = exact(gram, gram)
    bend = 1.6875 * eye - 0.5625 * gram + 0.0625 * twice
    total = 2.25 * eye - 2.4375 * gram + exact(twice, bend)
    energy = jnp.sum(gram * eye, keepdims=True)
    mean = jnp.sum(gram * total, keepdims=True) / jnp.maximum(energy, 1e-30)
    rest = ((total - mean * eye) * scale).astype(bf16)
    mean = mean * scale

    def finish(c, carry):
        load(c).wait()
        grad = grads[c].reshape(SLAB * chi, chi)
        done = (mean * grad + mm(grad.astype(bf16), rest)).astype(bf16)
        held[c] = jnp.transpose(done.reshape(SLAB, chi, chi), (1, 0, 2))
        pltpu.make_async_copy(
            held.at[c], out_ref.at[:, pl.ds(pl.multiple_of(c * SLAB, SLAB), SLAB), :], out_sem.at[c]
        ).start()
        return carry

    lax.fori_loop(0, held.shape[0], finish, 0)
    env_in.wait()
    env_back.start()
    for c in range(held.shape[0]):
        pltpu.make_async_copy(
            held.at[c], out_ref.at[:, pl.ds(c * SLAB, SLAB), :], out_sem.at[c]
        ).wait()
    env_back.wait()


def body(iso, edge_left, edge_right, coupling):
    iso = iso[0]
    chi, depth, _ = iso.shape
    blk = lax.axis_size("blk")
    bond = lax.axis_size("bond")
    levels = blk.bit_length() - 1
    square = (chi, chi)
    piece = chi // bond
    chunks = depth // SLAB
    half = chunks // 2
    work = 2 * depth * chi**3
    dma = pltpu.SemaphoreType.DMA
    hbm = pl.BlockSpec(memory_space=pltpu.HBM)
    grad, environ, grams, traces = pl.pallas_call(
        functools.partial(sweep_kernel, blk, bond, levels),
        in_specs=[hbm] * 4,
        out_specs=[hbm] * 4,
        out_shape=[
            jax.ShapeDtypeStruct((chunks, SLAB, *square), f32),
            jax.ShapeDtypeStruct((bond, piece, chi), f32),
            jax.ShapeDtypeStruct((bond, chi // 2, chi + chi // 2), bf16),
            jax.ShapeDtypeStruct((bond, 8, 128), f32),
        ],
        scratch_shapes=[
            pltpu.VMEM(square, bf16),
            pltpu.VMEM(square, bf16),
            pltpu.VMEM(square, f32),
            pltpu.VMEM((chunks, SLAB, *square), f32),
            pltpu.VMEM((min(4, chunks), chi, SLAB, chi), bf16),
            pltpu.VMEM((half + 1, SLAB, *square), bf16),
            pltpu.VMEM((half + 1, SLAB, *square), bf16),
            pltpu.VMEM((half + 1, chi, SLAB * chi), bf16),
            pltpu.VMEM((half + 1, chi, SLAB * chi), bf16),
            pltpu.VMEM((SLAB * chi, chi), bf16),
            pltpu.VMEM((SLAB * chi, chi), bf16),
            pltpu.VMEM((SLAB * chi, chi), bf16),
            pltpu.VMEM((SLAB * chi, chi), bf16),
            pltpu.VMEM((2, bond, piece, chi), f32),
            pltpu.VMEM((2, bond - 1, piece, chi), f32),
            pltpu.VMEM((2, bond, piece, chi), bf16),
            pltpu.VMEM((2, piece, chi), bf16),
            pltpu.VMEM((2, bond, piece, chi), bf16),
            pltpu.VMEM((bond, piece, chi), bf16),
            pltpu.VMEM((levels + 1, bond, piece, chi), f32),
            pltpu.VMEM((levels - 1, bond, piece, chi), f32),
            pltpu.VMEM((3, *square), f32),
            pltpu.VMEM((bond, chi // 2, chi + chi // 2), bf16),
            pltpu.VMEM((bond, 8, 128), f32),
            dma((min(4, chunks),)), dma((3,)), dma((chunks,)), dma((3,)),
            dma((2, bond - 1)), dma((2, bond - 1)),
            dma((2, bond - 1)), dma((2, bond - 1)),
            dma((2,)), dma((2,)), dma((2,)), dma((2,)),
            dma((bond - 1,)), dma((bond - 1,)),
            dma((levels - 1, 2)), dma((levels - 1, 2)),
            dma((levels - 1, bond - 1)), dma((levels - 1, bond - 1)),
            dma((bond - 1,)), dma((bond - 1,)),
            dma((bond - 1,)), dma((bond - 1,)),
        ],
        compiler_params=pltpu.CompilerParams(
            vmem_limit_bytes=SWEEP_VMEM, collective_id=0, has_side_effects=True
        ),
        cost_estimate=pl.CostEstimate(flops=10 * work, bytes_accessed=4 * iso.size, transcendentals=0),
        name="sweep",
    )(iso, edge_left[0], edge_right[0], coupling[0])
    updated, environ = pl.pallas_call(
        update_kernel,
        in_specs=[hbm] * 4,
        out_specs=[hbm] * 2,
        out_shape=[
            jax.ShapeDtypeStruct(iso.shape, bf16),
            jax.ShapeDtypeStruct((bond, piece, chi), f32),
        ],
        scratch_shapes=[
            pltpu.VMEM((chunks, SLAB, *square), f32),
            pltpu.VMEM((bond, piece, chi), f32),
            pltpu.VMEM((bond, chi // 2, chi + chi // 2), bf16),
            pltpu.VMEM((bond, 8, 128), f32),
            pltpu.VMEM((chunks, chi, SLAB, chi), bf16),
            dma((chunks,)), dma((chunks,)), dma((4,)),
        ],
        compiler_params=pltpu.CompilerParams(vmem_limit_bytes=UPDATE_VMEM),
        cost_estimate=pl.CostEstimate(flops=work, bytes_accessed=4 * iso.size, transcendentals=0),
        name="update",
    )(grad, environ, grams, traces)
    return (updated[None], environ.reshape(1, chi, chi))


def solution(mesh):
    placed = (
        P("blk", None, "bond", None),
        P("blk", None, None),
        P("blk", None, None),
        P("blk", None, None),
    )
    return jax.shard_map(
        body,
        mesh=mesh,
        in_specs=placed,
        out_specs=(P("blk", None, "bond", None), P("blk", None, None)),
        check_vma=False,
    )
```

```python
import functools

import jax
import jax.numpy as jnp
from jax import lax
from jax.experimental import pallas as pl
from jax.experimental.pallas import tpu as pltpu
from jax.sharding import PartitionSpec as P

GROUP = 4
SLAB = 8
SWEEP_VMEM = 40 * 1024 * 1024
UPDATE_VMEM = 20 * 1024 * 1024

f32 = jnp.float32
bf16 = jnp.bfloat16
MESH = pl.DeviceIdType.MESH


def mm(a, b):
    return jnp.dot(a, b, preferred_element_type=f32)


def turned_mm(a, b):
    return lax.dot_general(a, b, (((1,), (1,)), ((), ())), preferred_element_type=f32)


def product(a, b, times=mm):
    (ah, al), (bh, bl) = a, b
    return times(ah, bh) + (times(ah, bl) + times(al, bh))


def diagonal(shape):
    return lax.broadcasted_iota(jnp.int32, shape, 0) == lax.broadcasted_iota(jnp.int32, shape, 1)


def flipped(index, mask):
    out = index
    bit = 1
    while bit <= mask:
        if mask & bit:
            out = out + bit * (1 - 2 * lax.rem(index // bit, 2))
        bit *= 2
    return out


def halves(value):
    high = value.astype(bf16)
    return high, (value - high.astype(f32)).astype(bf16)


def sweep_kernel(
    blk, bond, levels,
    iso_ref, left_in, right_in, couple_in,
    grad_out, env_out, gram_out, trace_out,
    left_ref, right_ref, couple_ref, couple_high, couple_low, stage, even, odd, turn_even, turn_odd,
    high_even, low_even, high_odd, low_odd, total, heard, asc, around, other, mixed, envs, far, grams, packed, traces,
    in_sem, small_sem, rs_send, rs_recv, ag_send, ag_recv, nb_send, nb_recv, zero_send, zero_recv,
    mix_send, mix_recv, dir_send, dir_recv, fw_send, fw_recv, gr_send, gr_recv, tr_send, tr_recv,
):
    s = lax.axis_index("blk")
    r = lax.axis_index("bond")
    chi = left_ref.shape[0]
    chunks = iso_ref.shape[1] // SLAB
    slots_in = stage.shape[0]
    half = chunks // 2
    piece = chi // bond
    square = (chi, chi)
    cut = (bond, piece, chi)
    after = lax.rem(s + 1, blk)
    before = lax.rem(s + blk - 1, blk)
    masks = range(1, bond)
    pending = []

    def load(c):
        slot = lax.rem(c, slots_in)
        first = c * SLAB if isinstance(c, int) else pl.multiple_of(c * SLAB, SLAB)
        return pltpu.make_async_copy(
            iso_ref.at[:, pl.ds(first, SLAB), :], stage.at[slot], in_sem.at[slot]
        )

    small = [
        pltpu.make_async_copy(src, dst, small_sem.at[n])
        for n, (src, dst) in enumerate(
            ((left_in, left_ref), (right_in, right_ref), (couple_in, couple_ref))
        )
    ]
    load(0).start()
    for copy in small:
        copy.start()
    load(1).start()

    barrier = pltpu.get_barrier_semaphore()
    partners = [flipped(s, 1 << level) for level in range(levels)]
    greeted = [(s, flipped(r, mask)) for mask in masks]
    greeted += [(after, r), (before, r)] + [(t, r) for t in partners]
    for device in greeted:
        pl.semaphore_signal(barrier, inc=1, device_id=device, device_id_type=MESH)

    def send(src, dst, out_flag, in_flag, device):
        copy = pltpu.make_async_remote_copy(
            src_ref=src, dst_ref=dst, send_sem=out_flag, recv_sem=in_flag,
            device_id=device, device_id_type=MESH,
        )
        copy.start()
        pending.append(copy)
        return copy

    def relayout(c, dst, i):
        dst[i] = jnp.transpose(stage[lax.rem(c, slots_in)], (1, 0, 2))

    def spread(edge_ref, src, i, turn, high, low):
        for j in range(SLAB):
            one = src[i, j]
            place = slice(j * chi, (j + 1) * chi)
            high[place, :], low[place, :] = halves(mm(edge_ref[...], one))
            if turn is not None:
                turn[i, :, place] = one.T

    def collect(k, turn, i, high, low):
        turned = turn[i]
        total[k] += (mm(turned, high[...]) + mm(turned, low[...])).reshape(cut)

    even_parts = (high_even, low_even)
    odd_parts = (high_odd, low_odd)
    total[...] = jnp.zeros_like(total)
    grams[...] = jnp.zeros_like(grams)
    load(0).wait()
    for c in range(2, min(4, chunks)):
        load(c).start()
    for copy in small:
        copy.wait()
    couple_high[...], couple_low[...] = halves(couple_ref[...])
    relayout(0, even, 0)
    spread(left_ref, even, 0, turn_even, *even_parts)
    load(1).wait()
    relayout(1, odd, 0)

    def first_pass(i, carry):
        for ahead in (2, 3):
            @pl.when(2 * i + ahead < chunks)
            def _():
                load(2 * i + ahead).wait()

            @pl.when(2 * i + ahead + 2 < chunks)
            def _():
                load(2 * i + ahead + 2).start()

        collect(0, turn_even, i, *even_parts)
        spread(left_ref, odd, i, turn_odd, *odd_parts)
        relayout(2 * i + 2, even, i + 1)
        collect(0, turn_odd, i, *odd_parts)
        spread(left_ref, even, i + 1, turn_even, *even_parts)
        relayout(2 * i + 3, odd, i + 1)
        return carry

    with jax.named_scope('first'):
        lax.fori_loop(0, half, first_pass, 0)
    pl.semaphore_wait(barrier, len(greeted))

    def scatter(k):
        return [
            send(total.at[k, flipped(r, mask)], heard.at[k, mask - 1],
                 rs_send.at[k, mask - 1], rs_recv.at[k, mask - 1], (s, flipped(r, mask)))
            for mask in masks
        ]

    def gather(k):
        return [
            send(asc.at[k, r], asc.at[k, r], ag_send.at[k, mask - 1], ag_recv.at[k, mask - 1],
                 (s, flipped(r, mask)))
            for mask in masks
        ]

    def reduced(k, copies):
        for copy in copies:
            copy.wait_recv()
        own = total[k, r]
        for mask in masks:
            own = own + heard[k, mask - 1]
        asc[k, r] = own.astype(bf16)

    def arrived(copies):
        for copy in copies:
            copy.wait_recv()

    def second_pass(i, carry):
        collect(1, turn_even, i, *even_parts)
        spread(right_ref, odd, i, None, *odd_parts)
        collect(1, turn_odd, i, *odd_parts)
        spread(right_ref, even, i + 1, None, *even_parts)
        return carry

    scattered_left = scatter(0)
    spread(right_ref, even, 0, None, *even_parts)
    early = half * 3 // 4
    with jax.named_scope('second_a'):
        lax.fori_loop(0, early, second_pass, 0)
    with jax.named_scope('w_rs0'):
        reduced(0, scattered_left)
    gathered_left = gather(0)
    to_before = send(asc.at[0, r], around.at[0], nb_send.at[0], nb_recv.at[0], (before, r))
    with jax.named_scope('second_b'):
        lax.fori_loop(early, half, second_pass, 0)
    scattered_right = scatter(1)

    def plain_pass(i, carry):
        for src, turn in ((even, turn_even), (odd, turn_odd)):
            grams[2] += mm(turn[i], src[i].reshape(SLAB * chi, chi))
        return carry

    plain_early = half // 2
    with jax.named_scope('plain'):
        lax.fori_loop(0, plain_early, plain_pass, 0)
    with jax.named_scope('w_ag0'):
        arrived(gathered_left)
    zero_left = send(asc.at[0], other.at[0], zero_send.at[0], zero_recv.at[0], (partners[0], r))
    with jax.named_scope('w_rs1'):
        reduced(1, scattered_right)
    gathered_right = gather(1)
    to_after = send(asc.at[1, r], around.at[1], nb_send.at[1], nb_recv.at[1], (after, r))
    with jax.named_scope('w_ag1'):
        arrived(gathered_right)
    zero_right = send(asc.at[1], other.at[1], zero_send.at[1], zero_recv.at[1], (partners[0], r))
    envs[0] = asc[0].astype(f32) + asc[1].astype(f32)
    def climb(level, partner):
        couple = (couple_high[...], couple_low[...])
        carried = product(halves(product(couple, halves(partner.reshape(square)))), couple, turned_mm)
        envs[level + 1] = 0.5 * (envs[level] + carried.reshape(cut))

    with jax.named_scope('w_zero'):
        arrived([zero_left, zero_right])
    with jax.named_scope('climb0'):
        climb(0, other[0].astype(f32) + other[1].astype(f32))
    opposite = bond - 1

    def send_direct(level):
        return [
            send(envs.at[level, place], far.at[level - 1, place],
                 dir_send.at[level - 1, n], dir_recv.at[level - 1, n], (partners[level], r))
            for n, place in enumerate((r, flipped(r, opposite)))
        ]

    direct = send_direct(1)
    with jax.named_scope('w_nb'):
        arrived([to_before, to_after])
    mine = left_ref[pl.ds(pl.multiple_of(r * piece, piece), piece), :].astype(f32)
    mixed[r] = (mine + around[1].astype(f32) + around[0].astype(f32)).astype(bf16)
    gathered_mix = [
        send(mixed.at[r], mixed.at[r], mix_send.at[mask - 1], mix_recv.at[mask - 1],
             (s, flipped(r, mask)))
        for mask in masks
    ]

    def gram_pass(i, carry):
        mix = mixed[...].reshape(square)
        for src in (even, odd):
            for first in range(0, SLAB, GROUP):
                mats = [src[i, first + j] for j in range(GROUP)]
                rows = jnp.concatenate(mats, axis=0)
                moved = jnp.concatenate([mm(mix, one).astype(bf16) for one in mats], axis=0)
                turned = moved.T
                grams[0] += mm(turned, moved)
                grams[1] += mm(turned, rows)
        return carry

    weights = [1, 1] * (levels - 1)
    weights[0] = 0
    weights[-2] = 2
    bounds = [sum(weights[:n]) * half // sum(weights) for n in range(len(weights) + 1)]

    def gram_share(n):
        lax.fori_loop(bounds[n], bounds[n + 1], gram_pass, 0)

    for level in range(1, levels):
        if level == 1:
            with jax.named_scope('plain_late'):
                lax.fori_loop(plain_early, half, plain_pass, 0)
        else:
            direct = send_direct(level)
            with jax.named_scope('slot_a'):
                gram_share(2 * level - 2)
        with jax.named_scope('w_dir'):
            direct[0].wait_recv()
        passed = [
            send(far.at[level - 1, r], far.at[level - 1, r],
                 fw_send.at[level - 1, mask - 1], fw_recv.at[level - 1, mask - 1],
                 (s, flipped(r, mask)))
            for mask in masks if mask != opposite
        ]
        if level == 1:
            with jax.named_scope('w_mix'):
                arrived(gathered_mix)
        with jax.named_scope('slot_b'):
            gram_share(2 * level - 1)
        with jax.named_scope('w_dir1'):
            direct[1].wait_recv()
        with jax.named_scope('w_fw'):
            arrived(passed)
        with jax.named_scope('climb'):
            climb(level, far[level - 1])

    env = envs[levels].reshape(square)
    top = env.astype(bf16)
    flip = top.T
    high, low = halves(grams[2])
    high, low = halves(grams[1] + 0.5 * (mm(flip, high) + mm(flip, low)))
    crossed = mm(high, top) + mm(low, top)
    gram = grams[0] + crossed + crossed.T
    low = chi // 2
    packed[r] = jnp.concatenate([gram[:low], gram[low:, low:]], axis=1).astype(bf16)
    trace = jnp.sum(jnp.where(diagonal(gram.shape), gram, 0.0), keepdims=True)
    traces[r] = jnp.broadcast_to(trace, traces.shape[1:])
    gathered_gram = []
    for mask in masks:
        device = (s, flipped(r, mask))
        gathered_gram.append(send(
            packed.at[r], packed.at[r], gr_send.at[mask - 1], gr_recv.at[mask - 1], device))
        gathered_gram.append(send(
            traces.at[r], traces.at[r], tr_send.at[mask - 1], tr_recv.at[mask - 1], device))
    env_out[...] = envs[levels]

    def grad_pass(i, carry):
        mix = mixed[...].reshape(square)
        for n, src in enumerate((even, odd)):
            moved = jnp.concatenate([mm(mix, src[i, j]) for j in range(SLAB)], axis=0)
            whole = moved + mm(src[i].reshape(SLAB * chi, chi), top)
            grad_out[2 * i + n] = jnp.transpose(whole.reshape(SLAB, chi, chi), (1, 0, 2))
        return carry

    with jax.named_scope('grad'):
        lax.fori_loop(0, half, grad_pass, 0)
    with jax.named_scope('w_gram'):
        arrived(gathered_gram)
    gram_out[...] = packed[...]
    trace_out[...] = traces[...]
    for copy in pending:
        copy.wait_send()


def update_kernel(
    grads, env_ref, gram_ref, trace_ref, out_ref, env_out, held, out_sem, env_sem
):
    env_back = pltpu.make_async_copy(env_ref, env_out, env_sem)
    env_back.start()
    chi = out_ref.shape[0]
    low = chi // 2
    packed = gram_ref[0].astype(f32)
    squares = trace_ref[0]
    for rank in range(1, gram_ref.shape[0]):
        packed = packed + gram_ref[rank].astype(f32)
        squares = squares + trace_ref[rank]
    scale = lax.rsqrt(squares[0:1, 0:1] + 1e-06)
    under = jnp.concatenate([packed[:, low:chi].T, packed[:, chi:]], axis=1)
    gram = jnp.concatenate([packed[:, :chi], under], axis=0) * (scale * scale)
    eye = diagonal(gram.shape).astype(f32)
    parts = halves(gram)
    twice = product(parts, parts)
    bend = 1.6875 * eye - 0.5625 * gram + 0.0625 * twice
    total = 2.25 * eye - 2.4375 * gram + product(halves(twice), halves(bend))
    energy = jnp.sum(gram * eye, keepdims=True)
    mean = jnp.sum(gram * total, keepdims=True) / jnp.maximum(energy, 1e-30)
    rest = ((total - mean * eye) * scale).astype(bf16)
    mean = mean * scale

    def finish(c, carry):
        grad = grads[c].reshape(SLAB * chi, chi)
        done = (mean * grad + mm(grad.astype(bf16), rest)).astype(bf16)
        held[c] = done.reshape(chi, SLAB, chi)
        pltpu.make_async_copy(
            held.at[c], out_ref.at[:, pl.ds(pl.multiple_of(c * SLAB, SLAB), SLAB), :], out_sem.at[c]
        ).start()
        return carry

    lax.fori_loop(0, held.shape[0], finish, 0)
    for c in range(held.shape[0]):
        pltpu.make_async_copy(
            held.at[c], out_ref.at[:, pl.ds(c * SLAB, SLAB), :], out_sem.at[c]
        ).wait()
    env_back.wait()


def in_hbm(array):
    return pltpu.with_memory_space_constraint(array, pltpu.HBM)


def body(iso, edge_left, edge_right, coupling):
    iso = iso[0]
    chi, depth, _ = iso.shape
    blk = lax.axis_size("blk")
    bond = lax.axis_size("bond")
    levels = blk.bit_length() - 1
    square = (chi, chi)
    piece = chi // bond
    chunks = depth // SLAB
    half = chunks // 2
    work = 2 * depth * chi**3
    dma = pltpu.SemaphoreType.DMA
    vmem = pl.BlockSpec(memory_space=pltpu.VMEM)
    hbm = pl.BlockSpec(memory_space=pltpu.HBM)
    grad, environ, grams, traces = pl.pallas_call(
        functools.partial(sweep_kernel, blk, bond, levels),
        in_specs=[hbm] * 4,
        out_specs=[vmem] * 4,
        out_shape=[
            pltpu.VMEM((chunks, chi, SLAB, chi), f32),
            pltpu.VMEM((bond, piece, chi), f32),
            pltpu.VMEM((bond, chi // 2, chi + chi // 2), bf16),
            pltpu.VMEM((bond, 8, 128), f32),
        ],
        scratch_shapes=[
            pltpu.VMEM(square, bf16),
            pltpu.VMEM(square, bf16),
            pltpu.VMEM(square, f32),
            pltpu.VMEM(square, bf16),
            pltpu.VMEM(square, bf16),
            pltpu.VMEM((min(4, chunks), chi, SLAB, chi), bf16),
            pltpu.VMEM((half + 1, SLAB, *square), bf16),
            pltpu.VMEM((half + 1, SLAB, *square), bf16),
            pltpu.VMEM((half + 1, chi, SLAB * chi), bf16),
            pltpu.VMEM((half + 1, chi, SLAB * chi), bf16),
            pltpu.VMEM((SLAB * chi, chi), bf16),
            pltpu.VMEM((SLAB * chi, chi), bf16),
            pltpu.VMEM((SLAB * chi, chi), bf16),
            pltpu.VMEM((SLAB * chi, chi), bf16),
            pltpu.VMEM((2, bond, piece, chi), f32),
            pltpu.VMEM((2, bond - 1, piece, chi), f32),
            pltpu.VMEM((2, bond, piece, chi), bf16),
            pltpu.VMEM((2, piece, chi), bf16),
            pltpu.VMEM((2, bond, piece, chi), bf16),
            pltpu.VMEM((bond, piece, chi), bf16),
            pltpu.VMEM((levels + 1, bond, piece, chi), f32),
            pltpu.VMEM((levels - 1, bond, piece, chi), f32),
            pltpu.VMEM((3, *square), f32),
            pltpu.VMEM((bond, chi // 2, chi + chi // 2), bf16),
            pltpu.VMEM((bond, 8, 128), f32),
            dma((min(4, chunks),)), dma((3,)),
            dma((2, bond - 1)), dma((2, bond - 1)),
            dma((2, bond - 1)), dma((2, bond - 1)),
            dma((2,)), dma((2,)), dma((2,)), dma((2,)),
            dma((bond - 1,)), dma((bond - 1,)),
            dma((levels - 1, 2)), dma((levels - 1, 2)),
            dma((levels - 1, bond - 1)), dma((levels - 1, bond - 1)),
            dma((bond - 1,)), dma((bond - 1,)),
            dma((bond - 1,)), dma((bond - 1,)),
        ],
        compiler_params=pltpu.CompilerParams(
            vmem_limit_bytes=SWEEP_VMEM, collective_id=0, has_side_effects=True
        ),
        cost_estimate=pl.CostEstimate(flops=10 * work, bytes_accessed=4 * iso.size, transcendentals=0),
        name="sweep",
    )(*map(in_hbm, (iso, edge_left[0], edge_right[0], coupling[0])))
    updated, environ = pl.pallas_call(
        update_kernel,
        in_specs=[vmem] * 4,
        out_specs=[hbm] * 2,
        out_shape=[
            jax.ShapeDtypeStruct(iso.shape, bf16),
            jax.ShapeDtypeStruct((bond, piece, chi), f32),
        ],
        scratch_shapes=[pltpu.VMEM((chunks, chi, SLAB, chi), bf16), dma((chunks,)), dma],
        compiler_params=pltpu.CompilerParams(vmem_limit_bytes=UPDATE_VMEM),
        cost_estimate=pl.CostEstimate(flops=work, bytes_accessed=4 * iso.size, transcendentals=0),
        name="update",
    )(grad, environ, grams, traces)
    return (updated[None], environ.reshape(1, chi, chi))


def solution(mesh):
    placed = (
        P("blk", None, "bond", None),
        P("blk", None, None),
        P("blk", None, None),
        P("blk", None, None),
    )
    return jax.shard_map(
        body,
        mesh=mesh,
        in_specs=placed,
        out_specs=(P("blk", None, "bond", None), P("blk", None, None)),
        check_vma=False,
    )
```

```python
import functools

import jax
import jax.numpy as jnp
from jax import lax
from jax.experimental import pallas as pl
from jax.experimental.pallas import tpu as pltpu
from jax.sharding import PartitionSpec as P

GROUP = 4
SLAB = 8
SWEEP_VMEM = 40 * 1024 * 1024
UPDATE_VMEM = 20 * 1024 * 1024

f32 = jnp.float32
bf16 = jnp.bfloat16
MESH = pl.DeviceIdType.MESH


def mm(a, b):
    return jnp.dot(a, b, preferred_element_type=f32)


def turned_mm(a, b):
    return lax.dot_general(a, b, (((1,), (1,)), ((), ())), preferred_element_type=f32)


def product(a, b, times=mm):
    (ah, al), (bh, bl) = a, b
    return times(ah, bh) + (times(ah, bl) + times(al, bh))


def diagonal(shape):
    return lax.broadcasted_iota(jnp.int32, shape, 0) == lax.broadcasted_iota(jnp.int32, shape, 1)


def flipped(index, mask):
    out = index
    bit = 1
    while bit <= mask:
        if mask & bit:
            out = out + bit * (1 - 2 * lax.rem(index // bit, 2))
        bit *= 2
    return out


def halves(value):
    high = value.astype(bf16)
    return high, (value - high.astype(f32)).astype(bf16)


def sweep_kernel(
    blk, bond, levels,
    iso_ref, left_in, right_in, couple_in,
    grad_out, env_out, gram_out, trace_out,
    left_ref, right_ref, couple_ref, couple_high, couple_low, stage, even, odd, turn_even, turn_odd,
    high_even, low_even, high_odd, low_odd, total, heard, asc, around, other, mixed, envs, far, grams, packed, traces,
    in_sem, small_sem, rs_send, rs_recv, ag_send, ag_recv, nb_send, nb_recv, zero_send, zero_recv,
    mix_send, mix_recv, dir_send, dir_recv, fw_send, fw_recv, gr_send, gr_recv, tr_send, tr_recv,
):
    s = lax.axis_index("blk")
    r = lax.axis_index("bond")
    chi = left_ref.shape[0]
    chunks = iso_ref.shape[1] // SLAB
    slots_in = stage.shape[0]
    half = chunks // 2
    piece = chi // bond
    square = (chi, chi)
    cut = (bond, piece, chi)
    after = lax.rem(s + 1, blk)
    before = lax.rem(s + blk - 1, blk)
    masks = range(bond - 1, 0, -1)
    pending = []

    def load(c):
        slot = lax.rem(c, slots_in)
        first = c * SLAB if isinstance(c, int) else pl.multiple_of(c * SLAB, SLAB)
        return pltpu.make_async_copy(
            iso_ref.at[:, pl.ds(first, SLAB), :], stage.at[slot], in_sem.at[slot]
        )

    small = [
        pltpu.make_async_copy(src, dst, small_sem.at[n])
        for n, (src, dst) in enumerate(
            ((left_in, left_ref), (right_in, right_ref), (couple_in, couple_ref))
        )
    ]
    load(0).start()
    for copy in small:
        copy.start()
    load(1).start()

    barrier = pltpu.get_barrier_semaphore()
    partners = [flipped(s, 1 << level) for level in range(levels)]
    greeted = [(s, flipped(r, mask)) for mask in masks]
    greeted += [(after, r), (before, r)] + [(t, r) for t in partners]
    for device in greeted:
        pl.semaphore_signal(barrier, inc=1, device_id=device, device_id_type=MESH)

    def send(src, dst, out_flag, in_flag, device):
        copy = pltpu.make_async_remote_copy(
            src_ref=src, dst_ref=dst, send_sem=out_flag, recv_sem=in_flag,
            device_id=device, device_id_type=MESH,
        )
        copy.start()
        pending.append(copy)
        return copy

    def relayout(c, dst, i):
        dst[i] = jnp.transpose(stage[lax.rem(c, slots_in)], (1, 0, 2))

    def spread(edge_ref, src, i, turn, high, low):
        for j in range(SLAB):
            one = src[i, j]
            place = slice(j * chi, (j + 1) * chi)
            high[place, :], low[place, :] = halves(mm(edge_ref[...], one))
            if turn is not None:
                turn[i, :, place] = one.T

    def collect(k, turn, i, high, low):
        turned = turn[i]
        total[k] += (mm(turned, high[...]) + mm(turned, low[...])).reshape(cut)

    even_parts = (high_even, low_even)
    odd_parts = (high_odd, low_odd)
    total[...] = jnp.zeros_like(total)
    grams[...] = jnp.zeros_like(grams)
    load(0).wait()
    for c in range(2, min(4, chunks)):
        load(c).start()
    for copy in small:
        copy.wait()
    couple_high[...], couple_low[...] = halves(couple_ref[...])
    relayout(0, even, 0)
    spread(left_ref, even, 0, turn_even, *even_parts)
    load(1).wait()
    relayout(1, odd, 0)

    def first_pass(i, carry):
        for ahead in (2, 3):
            @pl.when(2 * i + ahead < chunks)
            def _():
                load(2 * i + ahead).wait()

            @pl.when(2 * i + ahead + 2 < chunks)
            def _():
                load(2 * i + ahead + 2).start()

        collect(0, turn_even, i, *even_parts)
        spread(left_ref, odd, i, turn_odd, *odd_parts)
        relayout(2 * i + 2, even, i + 1)
        collect(0, turn_odd, i, *odd_parts)
        spread(left_ref, even, i + 1, turn_even, *even_parts)
        relayout(2 * i + 3, odd, i + 1)
        return carry

    with jax.named_scope('first'):
        lax.fori_loop(0, half, first_pass, 0)
    pl.semaphore_wait(barrier, len(greeted))

    def scatter(k):
        return [
            send(total.at[k, flipped(r, mask)], heard.at[k, mask - 1],
                 rs_send.at[k, mask - 1], rs_recv.at[k, mask - 1], (s, flipped(r, mask)))
            for mask in masks
        ]

    def gather(k):
        return [
            send(asc.at[k, r], asc.at[k, r], ag_send.at[k, mask - 1], ag_recv.at[k, mask - 1],
                 (s, flipped(r, mask)))
            for mask in masks
        ]

    def reduced(k, copies):
        for copy in copies:
            copy.wait_recv()
        own = total[k, r]
        for mask in masks:
            own = own + heard[k, mask - 1]
        asc[k, r] = own.astype(bf16)

    def arrived(copies):
        for copy in copies:
            copy.wait_recv()

    def second_pass(i, carry):
        collect(1, turn_even, i, *even_parts)
        spread(right_ref, odd, i, None, *odd_parts)
        collect(1, turn_odd, i, *odd_parts)
        spread(right_ref, even, i + 1, None, *even_parts)
        return carry

    scattered_left = scatter(0)
    spread(right_ref, even, 0, None, *even_parts)
    early = half * 3 // 4
    with jax.named_scope('second_a'):
        lax.fori_loop(0, early, second_pass, 0)
    with jax.named_scope('w_rs0'):
        reduced(0, scattered_left)
    gathered_left = gather(0)
    to_before = send(asc.at[0, r], around.at[0], nb_send.at[0], nb_recv.at[0], (before, r))
    with jax.named_scope('second_b'):
        lax.fori_loop(early, half, second_pass, 0)
    scattered_right = scatter(1)

    def plain_pass(i, carry):
        for src, turn in ((even, turn_even), (odd, turn_odd)):
            grams[2] += mm(turn[i], src[i].reshape(SLAB * chi, chi))
        return carry

    plain_early = half // 2
    with jax.named_scope('plain'):
        lax.fori_loop(0, plain_early, plain_pass, 0)
    with jax.named_scope('w_ag0'):
        arrived(gathered_left)
    zero_left = send(asc.at[0], other.at[0], zero_send.at[0], zero_recv.at[0], (partners[0], r))
    with jax.named_scope('w_rs1'):
        reduced(1, scattered_right)
    gathered_right = gather(1)
    to_after = send(asc.at[1, r], around.at[1], nb_send.at[1], nb_recv.at[1], (after, r))
    with jax.named_scope('w_ag1'):
        arrived(gathered_right)
    zero_right = send(asc.at[1], other.at[1], zero_send.at[1], zero_recv.at[1], (partners[0], r))
    envs[0] = asc[0].astype(f32) + asc[1].astype(f32)
    def climb(level, partner):
        couple = (couple_high[...], couple_low[...])
        carried = product(halves(product(couple, halves(partner.reshape(square)))), couple, turned_mm)
        envs[level + 1] = 0.5 * (envs[level] + carried.reshape(cut))

    with jax.named_scope('w_zero'):
        arrived([zero_left, zero_right])
    with jax.named_scope('climb0'):
        climb(0, other[0].astype(f32) + other[1].astype(f32))
    opposite = bond - 1

    def send_direct(level):
        return [
            send(envs.at[level, place], far.at[level - 1, place],
                 dir_send.at[level - 1, n], dir_recv.at[level - 1, n], (partners[level], r))
            for n, place in enumerate((r, flipped(r, opposite)))
        ]

    direct = send_direct(1)
    with jax.named_scope('w_nb'):
        arrived([to_before, to_after])
    mine = left_ref[pl.ds(pl.multiple_of(r * piece, piece), piece), :].astype(f32)
    mixed[r] = (mine + around[1].astype(f32) + around[0].astype(f32)).astype(bf16)
    gathered_mix = [
        send(mixed.at[r], mixed.at[r], mix_send.at[mask - 1], mix_recv.at[mask - 1],
             (s, flipped(r, mask)))
        for mask in masks
    ]

    def gram_pass(i, carry):
        mix = mixed[...].reshape(square)
        for src in (even, odd):
            for first in range(0, SLAB, GROUP):
                mats = [src[i, first + j] for j in range(GROUP)]
                rows = jnp.concatenate(mats, axis=0)
                moved = jnp.concatenate([mm(mix, one).astype(bf16) for one in mats], axis=0)
                turned = moved.T
                grams[0] += mm(turned, moved)
                grams[1] += mm(turned, rows)
        return carry

    weights = [1, 1] * (levels - 1)
    weights[0] = 0
    weights[-2] = 2
    bounds = [sum(weights[:n]) * half // sum(weights) for n in range(len(weights) + 1)]

    def gram_share(n):
        lax.fori_loop(bounds[n], bounds[n + 1], gram_pass, 0)

    for level in range(1, levels):
        if level == 1:
            with jax.named_scope('plain_late'):
                lax.fori_loop(plain_early, half, plain_pass, 0)
        else:
            direct = send_direct(level)
            with jax.named_scope('slot_a'):
                gram_share(2 * level - 2)
        with jax.named_scope('w_dir'):
            direct[0].wait_recv()
        passed = [
            send(far.at[level - 1, r], far.at[level - 1, r],
                 fw_send.at[level - 1, mask - 1], fw_recv.at[level - 1, mask - 1],
                 (s, flipped(r, mask)))
            for mask in masks if mask != opposite
        ]
        if level == 1:
            with jax.named_scope('w_mix'):
                arrived(gathered_mix)
        with jax.named_scope('slot_b'):
            gram_share(2 * level - 1)
        with jax.named_scope('w_dir1'):
            direct[1].wait_recv()
        with jax.named_scope('w_fw'):
            arrived(passed)
        with jax.named_scope('climb'):
            climb(level, far[level - 1])

    env = envs[levels].reshape(square)
    top = env.astype(bf16)
    flip = top.T
    high, low = halves(grams[2])
    high, low = halves(grams[1] + 0.5 * (mm(flip, high) + mm(flip, low)))
    crossed = mm(high, top) + mm(low, top)
    gram = grams[0] + crossed + crossed.T
    low = chi // 2
    packed[r] = jnp.concatenate([gram[:low], gram[low:, low:]], axis=1).astype(bf16)
    trace = jnp.sum(jnp.where(diagonal(gram.shape), gram, 0.0), keepdims=True)
    traces[r] = jnp.broadcast_to(trace, traces.shape[1:])
    gathered_gram = []
    for mask in masks:
        device = (s, flipped(r, mask))
        gathered_gram.append(send(
            packed.at[r], packed.at[r], gr_send.at[mask - 1], gr_recv.at[mask - 1], device))
        gathered_gram.append(send(
            traces.at[r], traces.at[r], tr_send.at[mask - 1], tr_recv.at[mask - 1], device))
    env_out[...] = envs[levels]

    def grad_pass(i, carry):
        mix = mixed[...].reshape(square)
        for n, src in enumerate((even, odd)):
            moved = jnp.concatenate([mm(mix, src[i, j]) for j in range(SLAB)], axis=0)
            whole = moved + mm(src[i].reshape(SLAB * chi, chi), top)
            grad_out[2 * i + n] = jnp.transpose(whole.reshape(SLAB, chi, chi), (1, 0, 2))
        return carry

    with jax.named_scope('grad'):
        lax.fori_loop(0, half, grad_pass, 0)
    with jax.named_scope('w_gram'):
        arrived(gathered_gram)
    gram_out[...] = packed[...]
    trace_out[...] = traces[...]
    for copy in pending:
        copy.wait_send()


def update_kernel(
    grads, env_ref, gram_ref, trace_ref, out_ref, env_out, held, out_sem, env_sem
):
    env_back = pltpu.make_async_copy(env_ref, env_out, env_sem)
    env_back.start()
    chi = out_ref.shape[0]
    low = chi // 2
    packed = gram_ref[0].astype(f32)
    squares = trace_ref[0]
    for rank in range(1, gram_ref.shape[0]):
        packed = packed + gram_ref[rank].astype(f32)
        squares = squares + trace_ref[rank]
    scale = lax.rsqrt(squares[0:1, 0:1] + 1e-06)
    under = jnp.concatenate([packed[:, low:chi].T, packed[:, chi:]], axis=1)
    gram = jnp.concatenate([packed[:, :chi], under], axis=0) * (scale * scale)
    eye = diagonal(gram.shape).astype(f32)
    parts = halves(gram)
    twice = product(parts, parts)
    bend = 1.6875 * eye - 0.5625 * gram + 0.0625 * twice
    total = 2.25 * eye - 2.4375 * gram + product(halves(twice), halves(bend))
    energy = jnp.sum(gram * eye, keepdims=True)
    mean = jnp.sum(gram * total, keepdims=True) / jnp.maximum(energy, 1e-30)
    rest = ((total - mean * eye) * scale).astype(bf16)
    mean = mean * scale

    def finish(c, carry):
        grad = grads[c].reshape(SLAB * chi, chi)
        done = (mean * grad + mm(grad.astype(bf16), rest)).astype(bf16)
        held[c] = done.reshape(chi, SLAB, chi)
        pltpu.make_async_copy(
            held.at[c], out_ref.at[:, pl.ds(pl.multiple_of(c * SLAB, SLAB), SLAB), :], out_sem.at[c]
        ).start()
        return carry

    lax.fori_loop(0, held.shape[0], finish, 0)
    for c in range(held.shape[0]):
        pltpu.make_async_copy(
            held.at[c], out_ref.at[:, pl.ds(c * SLAB, SLAB), :], out_sem.at[c]
        ).wait()
    env_back.wait()


def in_hbm(array):
    return pltpu.with_memory_space_constraint(array, pltpu.HBM)


def body(iso, edge_left, edge_right, coupling):
    iso = iso[0]
    chi, depth, _ = iso.shape
    blk = lax.axis_size("blk")
    bond = lax.axis_size("bond")
    levels = blk.bit_length() - 1
    square = (chi, chi)
    piece = chi // bond
    chunks = depth // SLAB
    half = chunks // 2
    work = 2 * depth * chi**3
    dma = pltpu.SemaphoreType.DMA
    vmem = pl.BlockSpec(memory_space=pltpu.VMEM)
    hbm = pl.BlockSpec(memory_space=pltpu.HBM)
    grad, environ, grams, traces = pl.pallas_call(
        functools.partial(sweep_kernel, blk, bond, levels),
        in_specs=[hbm] * 4,
        out_specs=[vmem] * 4,
        out_shape=[
            pltpu.VMEM((chunks, chi, SLAB, chi), f32),
            pltpu.VMEM((bond, piece, chi), f32),
            pltpu.VMEM((bond, chi // 2, chi + chi // 2), bf16),
            pltpu.VMEM((bond, 8, 128), f32),
        ],
        scratch_shapes=[
            pltpu.VMEM(square, bf16),
            pltpu.VMEM(square, bf16),
            pltpu.VMEM(square, f32),
            pltpu.VMEM(square, bf16),
            pltpu.VMEM(square, bf16),
            pltpu.VMEM((min(4, chunks), chi, SLAB, chi), bf16),
            pltpu.VMEM((half + 1, SLAB, *square), bf16),
            pltpu.VMEM((half + 1, SLAB, *square), bf16),
            pltpu.VMEM((half + 1, chi, SLAB * chi), bf16),
            pltpu.VMEM((half + 1, chi, SLAB * chi), bf16),
            pltpu.VMEM((SLAB * chi, chi), bf16),
            pltpu.VMEM((SLAB * chi, chi), bf16),
            pltpu.VMEM((SLAB * chi, chi), bf16),
            pltpu.VMEM((SLAB * chi, chi), bf16),
            pltpu.VMEM((2, bond, piece, chi), f32),
            pltpu.VMEM((2, bond - 1, piece, chi), f32),
            pltpu.VMEM((2, bond, piece, chi), bf16),
            pltpu.VMEM((2, piece, chi), bf16),
            pltpu.VMEM((2, bond, piece, chi), bf16),
            pltpu.VMEM((bond, piece, chi), bf16),
            pltpu.VMEM((levels + 1, bond, piece, chi), f32),
            pltpu.VMEM((levels - 1, bond, piece, chi), f32),
            pltpu.VMEM((3, *square), f32),
            pltpu.VMEM((bond, chi // 2, chi + chi // 2), bf16),
            pltpu.VMEM((bond, 8, 128), f32),
            dma((min(4, chunks),)), dma((3,)),
            dma((2, bond - 1)), dma((2, bond - 1)),
            dma((2, bond - 1)), dma((2, bond - 1)),
            dma((2,)), dma((2,)), dma((2,)), dma((2,)),
            dma((bond - 1,)), dma((bond - 1,)),
            dma((levels - 1, 2)), dma((levels - 1, 2)),
            dma((levels - 1, bond - 1)), dma((levels - 1, bond - 1)),
            dma((bond - 1,)), dma((bond - 1,)),
            dma((bond - 1,)), dma((bond - 1,)),
        ],
        compiler_params=pltpu.CompilerParams(
            vmem_limit_bytes=SWEEP_VMEM, collective_id=0, has_side_effects=True
        ),
        cost_estimate=pl.CostEstimate(flops=10 * work, bytes_accessed=4 * iso.size, transcendentals=0),
        name="sweep",
    )(*map(in_hbm, (iso, edge_left[0], edge_right[0], coupling[0])))
    updated, environ = pl.pallas_call(
        update_kernel,
        in_specs=[vmem] * 4,
        out_specs=[hbm] * 2,
        out_shape=[
            jax.ShapeDtypeStruct(iso.shape, bf16),
            jax.ShapeDtypeStruct((bond, piece, chi), f32),
        ],
        scratch_shapes=[pltpu.VMEM((chunks, chi, SLAB, chi), bf16), dma((chunks,)), dma],
        compiler_params=pltpu.CompilerParams(vmem_limit_bytes=UPDATE_VMEM),
        cost_estimate=pl.CostEstimate(flops=work, bytes_accessed=4 * iso.size, transcendentals=0),
        name="update",
    )(grad, environ, grams, traces)
    return (updated[None], environ.reshape(1, chi, chi))


def solution(mesh):
    placed = (
        P("blk", None, "bond", None),
        P("blk", None, None),
        P("blk", None, None),
        P("blk", None, None),
    )
    return jax.shard_map(
        body,
        mesh=mesh,
        in_specs=placed,
        out_specs=(P("blk", None, "bond", None), P("blk", None, None)),
        check_vma=False,
    )
```
